64 devices in a mesh: rep: 4 (over x, y), data: 16 (over z, core).
Axes of the slice: x: 2, y: 2, z: 8, core: 2. Of those that a mesh axis runs over, the one named last changes fastest.
The devices are a block of a 4x4x8 slice.
Arguments:
- hidden: bfloat16 [8192, 1536], P(('rep', 'data')), parts along dimension 0
- adapter_id: int32 [8192], P(('rep', 'data')), parts along dimension 0
- w_gate: bfloat16 [1536, 8960], replicated
- w_up: bfloat16 [1536, 8960], replicated
- w_down: bfloat16 [8960, 1536], replicated
- a_gate: bfloat16 [128, 1536, 16], replicated
- b_gate: bfloat16 [128, 16, 8960], P('data')
- a_up: bfloat16 [128, 1536, 16], replicated
- b_up: bfloat16 [128, 16, 8960], P('data')
- a_down: bfloat16 [128, 8960, 16], replicated
- b_down: bfloat16 [128, 16, 1536], P('data')
Outputs:
- output: bfloat16 [8192, 1536], P(('rep', 'data')), parts along dimension 0
There are 4 independent parts. The reference program is written for one: setup_inputs(seed, part) draws one part's arguments, and reference() takes and returns one part's arrays. A program takes and returns all parts, laid end to end along the dimension named above; an argument that names none is the same for every part.
All inputs are finite; a program needn't handle non-finite values.
Results may differ from the reference program's by a relative error of at most 0.00623724.
Values are sent between devices in bfloat16 or wider.
A program may use at most 768 MiB of HBM per device.

```python
import jax
import jax.numpy as jnp
from jax import lax

D = 1536
FF = 8960
RANK = 16
ADAPTERS = 128
GROUP = 16
TOKENS_DEV = 128
TOKENS = 2048
CAP = 32
PER_OWNER = ADAPTERS // GROUP
ROW_BLOCK = min(64, TOKENS)
LORA_SCALE = 2.0


def draw_ids(key):
    key_hot, key_src, key_one, key_two = jax.random.split(key, 4)
    hot_owner = jax.random.randint(key_hot, (), 0, GROUP)

    def one_source(src_key):
        key_slot, key_order = jax.random.split(src_key)
        slot_order = jax.random.permutation(key_slot, (GROUP - 1) * (CAP - 1))
        extra_rank = slot_order[:TOKENS_DEV - CAP - GROUP + 1] // (CAP - 1)
        other_rank = jnp.concatenate([jnp.arange(GROUP - 1, dtype=jnp.int32), extra_rank.astype(jnp.int32)])
        other_owner = other_rank + (other_rank >= hot_owner).astype(jnp.int32)
        owner_ids = jnp.concatenate([jnp.full((CAP,), hot_owner, jnp.int32), other_owner])
        return jax.random.permutation(key_order, owner_ids)

    owner_ids = jax.vmap(one_source)(jax.random.split(key_src, GROUP)).reshape(TOKENS)
    pick_one = jax.random.randint(key_one, (TOKENS,), 0, PER_OWNER)
    pick_two = jax.random.randint(key_two, (TOKENS,), 0, PER_OWNER)
    return (owner_ids * PER_OWNER + jnp.minimum(pick_one, pick_two)).astype(jnp.int32)


def weight(key, shape, scale):
    return (jax.random.normal(key, shape, jnp.float32) * scale).astype(jnp.bfloat16)


def setup_inputs(seed: int = 0, part: int = 0) -> dict:
    base_key = jax.random.key(seed)
    part_key = jax.random.fold_in(base_key, part)
    key_rows, key_ids = jax.random.split(part_key)
    keys = jax.random.split(base_key, 9)
    return {
        'hidden': jax.random.normal(key_rows, (TOKENS, D), jnp.float32).astype(jnp.bfloat16),
        'adapter_id': draw_ids(key_ids),
        'w_gate': weight(keys[0], (D, FF), D ** -0.5),
        'w_up': weight(keys[1], (D, FF), D ** -0.5),
        'w_down': weight(keys[2], (FF, D), FF ** -0.5),
        'a_gate': weight(keys[3], (ADAPTERS, D, RANK), D ** -0.5),
        'b_gate': weight(keys[4], (ADAPTERS, RANK, FF), 0.15 * RANK ** -0.5),
        'a_up': weight(keys[5], (ADAPTERS, D, RANK), D ** -0.5),
        'b_up': weight(keys[6], (ADAPTERS, RANK, FF), 0.15 * RANK ** -0.5),
        'a_down': weight(keys[7], (ADAPTERS, FF, RANK), FF ** -0.5),
        'b_down': weight(keys[8], (ADAPTERS, RANK, D), 0.25 * RANK ** -0.5),
    }


def lora_delta(act_rows, a_rows, b_rows):
    low_rows = jnp.einsum('tk,tkr->tr', act_rows.astype(jnp.float32), a_rows.astype(jnp.float32)).astype(jnp.bfloat16)
    full_rows = jnp.einsum('tr,trm->tm', low_rows.astype(jnp.float32), b_rows.astype(jnp.float32))
    return (LORA_SCALE * full_rows).astype(jnp.bfloat16)


def reference(hidden, adapter_id, w_gate, w_up, w_down, a_gate, b_gate, a_up, b_up, a_down, b_down):
    def one_block(block):
        block_rows, block_ids = block
        gate_act = jnp.dot(block_rows, w_gate, preferred_element_type=jnp.float32) + lora_delta(block_rows, a_gate[block_ids], b_gate[block_ids]).astype(jnp.float32)
        up_act = jnp.dot(block_rows, w_up, preferred_element_type=jnp.float32) + lora_delta(block_rows, a_up[block_ids], b_up[block_ids]).astype(jnp.float32)
        hid_act = (jax.nn.silu(gate_act) * up_act).astype(jnp.bfloat16)
        down_act = jnp.dot(hid_act, w_down, preferred_element_type=jnp.float32) + lora_delta(hid_act, a_down[block_ids], b_down[block_ids]).astype(jnp.float32)
        return (block_rows.astype(jnp.float32) + down_act).astype(jnp.bfloat16)

    out_blocks = lax.map(one_block, (hidden.reshape(TOKENS // ROW_BLOCK, ROW_BLOCK, D), adapter_id.reshape(TOKENS // ROW_BLOCK, ROW_BLOCK)))
    return out_blocks.reshape(TOKENS, D)
```

```python
import jax
import jax.numpy as jnp
from jax import lax
from jax.sharding import PartitionSpec as P

scale_s = 2.0


def solution(mesh):
    groups = mesh.shape['data']
    row_spec = P(('rep', 'data'), None)
    tok_spec = P(('rep', 'data'))
    full_two = P(None, None)
    full_three = P(None, None, None)
    owned = P('data', None, None)

    def device_fn(hidden, adapter_id, w_gate, w_up, w_down, a_gate, b_gate, a_up, b_up, a_down, b_down):
        tok = hidden.shape[0]
        per_owner, rank, ff = b_gate.shape
        width = per_owner * rank
        cap = min(4 * tok // groups, tok // 2)
        me = lax.axis_index('data')
        owner = adapter_id // per_owner
        same = (owner[:, None] == owner[None, :]) & (jnp.arange(tok)[None, :] < jnp.arange(tok)[:, None])
        slot = owner * cap + jnp.sum(same.astype(jnp.int32), axis=1)
        place = (jnp.arange(groups * cap)[:, None] == slot[None, :])
        send_x = jnp.dot(place.astype(jnp.bfloat16), hidden, preferred_element_type=jnp.float32).astype(jnp.bfloat16)
        send_id = jnp.sum(jnp.where(place, (adapter_id % per_owner + 1)[None, :], 0), axis=1) - 1
        xs = lax.all_to_all(send_x, 'data', 0, 0, tiled=True)
        ids = lax.all_to_all(send_id, 'data', 0, 0, tiled=True)
        mask = (ids[:, None] == jnp.arange(width)[None, :] // rank)

        def mine(a):
            return lax.dynamic_slice_in_dim(a, me * per_owner, per_owner, 0)

        def delta(act, a, b):
            low = jnp.einsum('tk,akr->tar', act, mine(a), preferred_element_type=jnp.float32).reshape(-1, width)
            low = jnp.where(mask, low, 0.0).astype(jnp.bfloat16)
            full = jnp.dot(low, b.reshape(width, -1), preferred_element_type=jnp.float32)
            return (scale_s * full).astype(jnp.bfloat16).astype(jnp.float32)

        g = jnp.dot(xs, w_gate, preferred_element_type=jnp.float32) + delta(xs, a_gate, b_gate)
        u = jnp.dot(xs, w_up, preferred_element_type=jnp.float32) + delta(xs, a_up, b_up)
        h = (jax.nn.silu(g) * u).astype(jnp.bfloat16)
        y = jnp.dot(h, w_down, preferred_element_type=jnp.float32) + delta(h, a_down, b_down)
        out = (xs.astype(jnp.float32) + y).astype(jnp.bfloat16)
        back = lax.all_to_all(out, 'data', 0, 0, tiled=True)
        return lax.dot_general(place.astype(jnp.bfloat16), back, (((0,), (0,)), ((), ())), preferred_element_type=jnp.float32).astype(jnp.bfloat16)

    return jax.shard_map(device_fn, mesh=mesh, in_specs=(row_spec, tok_spec, full_two, full_two, full_two, full_three, owned, full_three, owned, full_three, owned), out_specs=row_spec, check_vma=False)
```

```python
import functools

import jax
import jax.numpy as jnp
from jax import lax
from jax.experimental import pallas as pl
from jax.experimental.pallas import tpu as pltpu
from jax.sharding import PartitionSpec as P

lora_scale = 2.0
col = 256
n_blocks = 7
n_slots = 4
same_rows = 32


def ring_order(chips):
    order = [0]
    for step in range(1, chips // 2):
        order += [step, chips - step]
    return order + [chips // 2]


def mlp_kernel(chips, rank, cross_rows, x_ref, id_ref, wg_ref, wu_ref, wd_ref, ag_ref, au_ref, ad_ref, bg_ref, bu_ref, bd_ref,
               o_ref, flag_ref, pg_ref, pu_ref, pd_ref,
               pool, xs, send, ret, hid, lowg, lowu, mask, ag, au, ad, bd, info,
               load_sem, wd_sem, small_sem, pair_sem, x_send, x_recv, info_send, info_recv, out_send, out_recv):
    order = ring_order(chips)
    position = {step: place for place, step in enumerate(order)}
    tok, depth = x_ref.shape
    width = bg_ref.shape[0]
    ff = wg_ref.shape[1]
    block = ff // n_blocks
    n_sub = block // col
    piece = depth + 2 * width
    used = 2 * n_sub * piece
    unit = same_rows + cross_rows
    rows = chips * unit
    half = rows // 2
    n_cols = depth // col
    per_slot = pool.shape[1] // ff
    f32, bf16 = jnp.float32, jnp.bfloat16

    me = lax.axis_index('data')
    core = lax.rem(me, 2)
    chip = me // 2
    partner = me + 1 - 2 * core
    targets = []
    for step in order:
        far = lax.rem(chip + step, chips)
        targets.append((2 * far + core, 2 * far + 1 - core))
    peers = [t for pair in targets for t in pair][1:]

    barrier = pltpu.get_barrier_semaphore()
    for peer in peers:
        pl.semaphore_signal(barrier, inc=1, device_id={'data': peer}, device_id_type=pl.DeviceIdType.MESH)

    def block_copies(b, slot, part):
        out = []
        for j in range(n_sub):
            cols = pl.ds(pl.multiple_of(b * block + j * col, col), col)
            for which, (w, own, far) in enumerate(((wg_ref, bg_ref, pg_ref), (wu_ref, bu_ref, pu_ref))):
                base = (2 * j + which) * piece
                if part != 'pair':
                    out.append((w.at[:, cols], pool.at[slot, pl.ds(base, depth)]))
                    out.append((own.at[:, cols], pool.at[slot, pl.ds(base + depth, width)]))
                if part != 'own':
                    out.append((far.at[:, cols], pool.at[slot, pl.ds(base + depth + width, width)]))
        for src, dst in out:
            pltpu.make_async_copy(src, dst, load_sem.at[slot]).start()

    def load_wait(slot):
        whole = pool.at[slot, pl.ds(0, used)]
        pltpu.make_async_copy(whole, whole, load_sem.at[slot]).wait()

    def remote(src, dst, s_sem, r_sem, dev):
        return pltpu.make_async_remote_copy(src_ref=src, dst_ref=dst, send_sem=s_sem, recv_sem=r_sem,
                                            device_id={'data': dev}, device_id_type=pl.DeviceIdType.MESH)

    for b in range(n_slots):
        block_copies(b, b, 'own')
    own_a = pl.ds(pl.multiple_of(me * width, width), width)
    far_a = pl.ds(pl.multiple_of(partner * width, width), width)
    for k, (src, dst) in enumerate(((ag_ref, ag), (au_ref, au), (ad_ref, ad))):
        pltpu.make_async_copy(src.at[own_a], dst.at[pl.ds(0, width)], small_sem.at[k]).start()
        pltpu.make_async_copy(src.at[far_a], dst.at[pl.ds(width, width)], small_sem.at[k]).start()
    pltpu.make_async_copy(bd_ref, bd.at[pl.ds(0, width)], small_sem.at[3]).start()

    ids = id_ref[...]
    tok_chip = ids // (2 * (width // rank))
    local = lax.rem(ids, 2 * (width // rank))
    step = lax.rem(tok_chip - chip + chips, chips)
    place = jnp.where(step < chips // 2, jnp.maximum(2 * step - 1, 0), jnp.where(step == chips // 2, chips - 1, 2 * (chips - step)))
    lanes = lax.broadcasted_iota(jnp.int32, (2 * chips, tok), 0)
    hot = (lanes == place).astype(f32)
    before = (lax.broadcasted_iota(jnp.int32, (tok, tok), 0) < lax.broadcasted_iota(jnp.int32, (tok, tok), 1))
    counts = jnp.dot(hot.astype(bf16), before.astype(f32).astype(bf16), preferred_element_type=f32)
    order_in = jnp.sum(hot * counts, axis=0, keepdims=True).astype(jnp.int32)
    over = order_in >= unit
    slot_of = jnp.where(over, rows + unit, place * unit + order_in)
    info[0] = slot_of * 32 + local
    perm = (lax.broadcasted_iota(jnp.int32, (rows, tok), 0) == slot_of).astype(f32).astype(bf16)
    send[...] = jnp.dot(perm, x_ref[...], preferred_element_type=f32).astype(bf16)
    xs[pl.ds(0, same_rows)] = send[pl.ds(0, same_rows)]

    pl.semaphore_wait(barrier, len(peers))

    for place_to, step_to in enumerate(order):
        seen = position[(chips - step_to) % chips]
        for kind in range(2):
            if place_to == 0 and kind == 0:
                continue
            remote(info.at[0], info.at[2 * seen + kind], info_send, info_recv, targets[place_to][kind]).start()
    pair_copies = [remote(src, dst, pair_sem.at[2 * k], pair_sem.at[2 * k + 1], partner)
                   for k, (src, dst) in enumerate(((bg_ref, pg_ref), (bu_ref, pu_ref), (bd_ref, pd_ref)))]
    for c in pair_copies:
        c.start()
    for place_to, step_to in enumerate(order):
        seen = position[(chips - step_to) % chips]
        for kind in range(2):
            if place_to == 0 and kind == 0:
                continue
            span = pl.ds(place_to * unit + kind * same_rows, cross_rows if kind else same_rows)
            land = pl.ds(seen * unit + kind * same_rows, cross_rows if kind else same_rows)
            remote(send.at[span], xs.at[land], x_send, x_recv.at[seen // (chips // 2)], targets[place_to][kind]).start()

    for c in pair_copies:
        c.wait()
    for b in range(n_slots):
        block_copies(b, b, 'pair')
    pltpu.make_async_copy(pd_ref, bd.at[pl.ds(width, width)], small_sem.at[3]).start()

    others = info.at[pl.ds(1, 2 * chips - 1)]
    pltpu.make_async_copy(others, others, info_recv).wait()
    flag = jnp.zeros((1, tok), jnp.int32)
    for seen, step_from in enumerate(order):
        theirs = position[(chips - step_from) % chips]
        for kind in range(2):
            code = info[2 * seen + kind]
            count = cross_rows if kind else same_rows
            slots = code // 32
            flag = jnp.maximum(flag, (slots >= rows).astype(jnp.int32))
            low_id = lax.rem(lax.rem(code, 32) + core * (width // rank), 2 * (width // rank))
            hit = lax.broadcasted_iota(jnp.int32, (count, tok), 0) + (theirs * unit + kind * same_rows) == slots
            pick = jnp.sum(jnp.where(hit, low_id + 1, 0), axis=1, keepdims=True)
            lane = lax.broadcasted_iota(jnp.int32, (count, 2 * width), 1) // rank + 1
            mask[pl.ds(seen * unit + kind * same_rows, count)] = (lane == pick).astype(f32).astype(bf16)
    flag_ref[...] = flag

    def low_rows(act, a, span):
        low = lax.dot_general(act, a[...], (((1,), (1,)), ((), ())), preferred_element_type=f32)
        return low.astype(bf16) * mask[span]

    def small_wait(k, dst):
        pltpu.make_async_copy(dst, dst, small_sem.at[k]).wait()

    def gate_up(b, span):
        slot = lax.rem(b, n_slots)
        act = xs[span]
        for j in range(n_sub):
            parts = []
            for which, low in enumerate((lowg, lowu)):
                base = (2 * j + which) * piece
                main = jnp.dot(act, pool[slot, pl.ds(base, depth)], preferred_element_type=f32)
                delta = jnp.dot(low[span], pool[slot, pl.ds(base + depth, 2 * width)], preferred_element_type=f32)
                parts.append(main + (lora_scale * delta).astype(bf16).astype(f32))
            gate, up = parts
            cols = pl.ds(pl.multiple_of(b * block + j * col, col), col)
            hid[span, cols] = (gate * jax.nn.sigmoid(gate) * up).astype(bf16)

    def x_wait(group, first):
        got = xs.at[pl.ds(first, (group + 1) * half - first)]
        pltpu.make_async_copy(got, got, x_recv.at[group]).wait()

    def wd_copy(j):
        slot = n_slots - 1 - j // per_slot
        start = (j % per_slot) * ff
        return pltpu.make_async_copy(wd_ref.at[:, pl.ds(pl.multiple_of(j * col, col), col)],
                                     pool.at[slot, pl.ds(start, ff)], wd_sem.at[j])

    near, far = pl.ds(0, half), pl.ds(half, half)
    small_wait(0, ag)
    small_wait(1, au)
    x_wait(0, same_rows)
    lowg[near] = low_rows(xs[near], ag, near)
    lowu[near] = low_rows(xs[near], au, near)

    @pl.loop(0, n_blocks)
    def _(b):
        load_wait(lax.rem(b, n_slots))
        gate_up(b, near)

        @pl.when(b < n_blocks - n_slots)
        def _():
            block_copies(b + n_slots, lax.rem(b, n_slots), 'all')

    x_wait(1, half)
    lowg[far] = low_rows(xs[far], ag, far)
    lowu[far] = low_rows(xs[far], au, far)

    @pl.loop(0, n_blocks)
    def _(i):
        b = n_blocks - 1 - i

        @pl.when(b < n_blocks - n_slots)
        def _():
            load_wait(lax.rem(b, n_slots))
        gate_up(b, far)

        @pl.when(i < n_blocks - n_slots)
        def _():
            block_copies(n_blocks - n_slots - 1 - i, lax.rem(b, n_slots), 'all')

        for k in range((n_cols + per_slot - 1) // per_slot):
            @pl.when(i == n_blocks - n_slots + k)
            def _():
                for j in range(k * per_slot, min((k + 1) * per_slot, n_cols)):
                    wd_copy(j).start()

    sent = send.at[pl.ds(same_rows, rows - same_rows)]
    pltpu.make_async_copy(sent, sent, x_send).wait()
    pltpu.make_async_copy(others, others, info_send).wait()
    small_wait(2, ad)
    small_wait(3, bd)
    every = pl.ds(0, rows)
    lowg[...] = low_rows(hid[...], ad, every)

    @pl.loop(0, n_cols)
    def _(j):
        slot = n_slots - 1 - j // per_slot
        start = pl.multiple_of(lax.rem(j, per_slot) * ff, 256)
        cols = pl.ds(pl.multiple_of(j * col, col), col)
        got = pool.at[slot, pl.ds(start, ff)]
        pltpu.make_async_copy(got, got, wd_sem.at[j]).wait()
        main = jnp.dot(hid[...], pool[slot, pl.ds(start, ff)], preferred_element_type=f32)
        delta = jnp.dot(lowg[...], bd[:, cols], preferred_element_type=f32)
        total = main + (lora_scale * delta).astype(bf16).astype(f32)
        send[:, cols] = (xs[:, cols].astype(f32) + total).astype(bf16)
        ret[pl.ds(0, same_rows), cols] = send[pl.ds(0, same_rows), cols]
        for seen in reversed(range(chips)):
            theirs = position[(chips - order[seen]) % chips]
            for kind in range(2):
                if seen == 0 and kind == 0:
                    continue
                count = cross_rows if kind else same_rows
                remote(send.at[pl.ds(seen * unit + kind * same_rows, count), cols],
                       ret.at[pl.ds(theirs * unit + kind * same_rows, count), cols],
                       out_send, out_recv, targets[seen][kind]).start()

    back = ret.at[pl.ds(same_rows, rows - same_rows)]
    pltpu.make_async_copy(back, back, out_recv).wait()
    o_ref[...] = lax.dot_general(perm, ret[...], (((0,), (0,)), ((), ())), preferred_element_type=f32).astype(bf16)
    pltpu.make_async_copy(sent, sent, out_send).wait()


def mlp_call(chips, rank, cross_rows, ident, x, ids, wg, wu, wd, ag, au, ad, bg, bu, bd):
    tok, depth = x.shape
    width = bg.shape[0]
    ff = wg.shape[1]
    rows = chips * (same_rows + cross_rows)
    n_sub = ff // n_blocks // col
    n_cols = depth // col
    slot_rows = max(2 * n_sub * (depth + 2 * width), ff)
    hbm, vmem = pl.BlockSpec(memory_space=pl.ANY), pl.BlockSpec(memory_space=pltpu.VMEM)
    bf16 = jnp.bfloat16
    dma = pltpu.SemaphoreType.DMA
    macs = rows * (3 * depth * ff + 2 * width * (2 * ff + depth) + 2 * width * (2 * depth + ff))
    return pl.pallas_call(
        functools.partial(mlp_kernel, chips, rank, cross_rows),
        out_shape=(jax.ShapeDtypeStruct((tok, depth), bf16), jax.ShapeDtypeStruct((1, tok), jnp.int32),
                   jax.ShapeDtypeStruct(bg.shape, bf16), jax.ShapeDtypeStruct(bu.shape, bf16), jax.ShapeDtypeStruct(bd.shape, bf16)),
        in_specs=[vmem, vmem] + [hbm] * 9,
        out_specs=(vmem, vmem, hbm, hbm, hbm),
        scratch_shapes=[
            pltpu.VMEM((n_slots, slot_rows, col), bf16),
            pltpu.VMEM((rows, depth), bf16), pltpu.VMEM((rows, depth), bf16), pltpu.VMEM((rows, depth), bf16),
            pltpu.VMEM((rows, ff), bf16),
            pltpu.VMEM((rows, 2 * width), bf16), pltpu.VMEM((rows, 2 * width), bf16), pltpu.VMEM((rows, 2 * width), bf16),
            pltpu.VMEM((2 * width, depth), bf16), pltpu.VMEM((2 * width, depth), bf16), pltpu.VMEM((2 * width, ff), bf16),
            pltpu.VMEM((2 * width, depth), bf16),
            pltpu.VMEM((2 * chips, 1, tok), jnp.int32),
            dma((n_slots,)), dma((n_cols,)), dma((4,)), dma((6,)), dma, dma((2,)), dma, dma, dma, dma,
        ],
        compiler_params=pltpu.CompilerParams(collective_id=ident, has_side_effects=True, vmem_limit_bytes=66_900_000),
        cost_estimate=pl.CostEstimate(flops=2 * macs, bytes_accessed=6 * depth * ff, transcendentals=rows * ff),
        name='mlp_%d' % cross_rows,
    )(x, ids, wg, wu, wd, ag, au, ad, bg, bu, bd)


def solution(mesh):
    groups = mesh.shape['data']
    row_spec = P(('rep', 'data'), None)
    tok_spec = P(('rep', 'data'))
    full_two = P(None, None)
    full_three = P(None, None, None)
    owned = P('data', None, None)

    def device_fn(hidden, adapter_id, w_gate, w_up, w_down, a_gate, b_gate, a_up, b_up, a_down, b_down):
        rank = b_gate.shape[1]

        def rank_rows(a):
            return jnp.swapaxes(a, 1, 2).reshape(-1, a.shape[1])

        def flat(b):
            return b.reshape(-1, b.shape[2])

        args = (hidden, adapter_id.reshape(1, -1), w_gate, w_up, w_down, rank_rows(a_gate), rank_rows(a_up), rank_rows(a_down),
                flat(b_gate), flat(b_up), flat(b_down))
        fast, flag = mlp_call(groups // 2, rank, same_rows // 2, 0, *args)[:2]
        return lax.cond(jnp.max(flag) > 0, lambda *a: mlp_call(groups // 2, rank, same_rows, 1, *a)[0], lambda *a: fast, *args)

    return jax.shard_map(device_fn, mesh=mesh, in_specs=(row_spec, tok_spec, full_two, full_two, full_two, full_three, owned, full_three, owned, full_three, owned), out_specs=row_spec, check_vma=False)
```

```python
import functools

import jax
import jax.numpy as jnp
from jax import lax
from jax.experimental import pallas as pl
from jax.experimental.pallas import tpu as pltpu
from jax.sharding import PartitionSpec as P

lora_scale = 2.0
col = 256
n_blocks = 7
n_slots = 4
same_rows = 32


def ring_order(chips):
    order = [0]
    for step in range(1, chips // 2):
        order += [step, chips - step]
    return order + [chips // 2]


def mlp_kernel(chips, rank, cross_rows, x_ref, id_ref, wg_ref, wu_ref, wd_ref, ag_ref, au_ref, ad_ref, bg_ref, bu_ref, bd_ref,
               o_ref, flag_ref, pg_ref, pu_ref, pd_ref,
               pool, xs, send, ret, hid, lowg, lowu, mask, ag, au, ad, bd, info,
               load_sem, wd_sem, small_sem, pair_sem, x_send, x_recv, info_send, info_recv, out_send, out_recv):
    order = ring_order(chips)
    position = {step: place for place, step in enumerate(order)}
    tok, depth = x_ref.shape
    width = bg_ref.shape[0]
    ff = wg_ref.shape[1]
    block = ff // n_blocks
    n_sub = block // col
    piece = depth + 2 * width
    used = 2 * n_sub * piece
    unit = same_rows + cross_rows
    rows = chips * unit
    half = rows // 2
    n_cols = depth // col
    per_slot = pool.shape[1] // ff
    f32, bf16 = jnp.float32, jnp.bfloat16

    me = lax.axis_index('data')
    core = lax.rem(me, 2)
    chip = me // 2
    partner = me + 1 - 2 * core
    targets = []
    for step in order:
        far = lax.rem(chip + step, chips)
        targets.append((2 * far + core, 2 * far + 1 - core))
    peers = [t for pair in targets for t in pair][1:]

    barrier = pltpu.get_barrier_semaphore()
    for peer in peers:
        pl.semaphore_signal(barrier, inc=1, device_id={'data': peer}, device_id_type=pl.DeviceIdType.MESH)

    def block_copies(b, slot, part):
        out = []
        for j in range(n_sub):
            cols = pl.ds(pl.multiple_of(b * block + j * col, col), col)
            for which, (w, own, far) in enumerate(((wg_ref, bg_ref, pg_ref), (wu_ref, bu_ref, pu_ref))):
                base = (2 * j + which) * piece
                if part != 'pair':
                    out.append((w.at[:, cols], pool.at[slot, pl.ds(base, depth)]))
                    out.append((own.at[:, cols], pool.at[slot, pl.ds(base + depth, width)]))
                if part != 'own':
                    out.append((far.at[:, cols], pool.at[slot, pl.ds(base + depth + width, width)]))
        for src, dst in out:
            pltpu.make_async_copy(src, dst, load_sem.at[slot]).start()

    def load_wait(slot):
        whole = pool.at[slot, pl.ds(0, used)]
        pltpu.make_async_copy(whole, whole, load_sem.at[slot]).wait()

    def remote(src, dst, s_sem, r_sem, dev):
        return pltpu.make_async_remote_copy(src_ref=src, dst_ref=dst, send_sem=s_sem, recv_sem=r_sem,
                                            device_id={'data': dev}, device_id_type=pl.DeviceIdType.MESH)

    for b in range(n_slots):
        block_copies(b, b, 'own')
    own_a = pl.ds(pl.multiple_of(me * width, width), width)
    far_a = pl.ds(pl.multiple_of(partner * width, width), width)
    for k, (src, dst) in enumerate(((ag_ref, ag), (au_ref, au), (ad_ref, ad))):
        pltpu.make_async_copy(src.at[own_a], dst.at[pl.ds(0, width)], small_sem.at[k]).start()
        pltpu.make_async_copy(src.at[far_a], dst.at[pl.ds(width, width)], small_sem.at[k]).start()
    pltpu.make_async_copy(bd_ref, bd.at[pl.ds(0, width)], small_sem.at[3]).start()

    ids = id_ref[...]
    tok_chip = ids // (2 * (width // rank))
    local = lax.rem(ids, 2 * (width // rank))
    step = lax.rem(tok_chip - chip + chips, chips)
    place = jnp.where(step < chips // 2, jnp.maximum(2 * step - 1, 0), jnp.where(step == chips // 2, chips - 1, 2 * (chips - step)))
    lanes = lax.broadcasted_iota(jnp.int32, (2 * chips, tok), 0)
    hot = (lanes == place).astype(f32)
    before = (lax.broadcasted_iota(jnp.int32, (tok, tok), 0) < lax.broadcasted_iota(jnp.int32, (tok, tok), 1))
    counts = jnp.dot(hot.astype(bf16), before.astype(f32).astype(bf16), preferred_element_type=f32)
    order_in = jnp.sum(hot * counts, axis=0, keepdims=True).astype(jnp.int32)
    over = order_in >= unit
    slot_of = jnp.where(over, rows + unit, place * unit + order_in)
    info[0] = slot_of * 32 + local
    perm = (lax.broadcasted_iota(jnp.int32, (rows, tok), 0) == slot_of).astype(f32).astype(bf16)
    send[...] = jnp.dot(perm, x_ref[...], preferred_element_type=f32).astype(bf16)
    xs[pl.ds(0, same_rows)] = send[pl.ds(0, same_rows)]

    pl.semaphore_wait(barrier, len(peers))

    for place_to, step_to in enumerate(order):
        seen = position[(chips - step_to) % chips]
        for kind in range(2):
            if place_to == 0 and kind == 0:
                continue
            remote(info.at[0], info.at[2 * seen + kind], info_send, info_recv, targets[place_to][kind]).start()
    pair_copies = [remote(src, dst, pair_sem.at[2 * k], pair_sem.at[2 * k + 1], partner)
                   for k, (src, dst) in enumerate(((bg_ref, pg_ref), (bu_ref, pu_ref), (bd_ref, pd_ref)))]
    for c in pair_copies:
        c.start()
    for place_to, step_to in enumerate(order):
        seen = position[(chips - step_to) % chips]
        for kind in range(2):
            if place_to == 0 and kind == 0:
                continue
            span = pl.ds(place_to * unit + kind * same_rows, cross_rows if kind else same_rows)
            land = pl.ds(seen * unit + kind * same_rows, cross_rows if kind else same_rows)
            remote(send.at[span], xs.at[land], x_send, x_recv.at[seen // (chips // 2)], targets[place_to][kind]).start()

    for c in pair_copies:
        c.wait()
    for b in range(n_slots):
        block_copies(b, b, 'pair')
    pltpu.make_async_copy(pd_ref, bd.at[pl.ds(width, width)], small_sem.at[3]).start()

    others = info.at[pl.ds(1, 2 * chips - 1)]
    pltpu.make_async_copy(others, others, info_recv).wait()
    flag = jnp.zeros((1, tok), jnp.int32)
    for seen, step_from in enumerate(order):
        theirs = position[(chips - step_from) % chips]
        for kind in range(2):
            code = info[2 * seen + kind]
            count = cross_rows if kind else same_rows
            slots = code // 32
            flag = jnp.maximum(flag, (slots >= rows).astype(jnp.int32))
            low_id = lax.rem(lax.rem(code, 32) + core * (width // rank), 2 * (width // rank))
            hit = lax.broadcasted_iota(jnp.int32, (count, tok), 0) + (theirs * unit + kind * same_rows) == slots
            pick = jnp.sum(jnp.where(hit, low_id + 1, 0), axis=1, keepdims=True)
            lane = lax.broadcasted_iota(jnp.int32, (count, 2 * width), 1) // rank + 1
            mask[pl.ds(seen * unit + kind * same_rows, count)] = (lane == pick).astype(f32).astype(bf16)
    flag_ref[...] = flag

    def low_rows(act, a, span):
        low = lax.dot_general(act, a[...], (((1,), (1,)), ((), ())), preferred_element_type=f32)
        return low.astype(bf16) * mask[span]

    def small_wait(k, dst):
        pltpu.make_async_copy(dst, dst, small_sem.at[k]).wait()

    def gate_up(b, span):
        slot = lax.rem(b, n_slots)
        act = xs[span]
        for j in range(n_sub):
            parts = []
            for which, low in enumerate((lowg, lowu)):
                base = (2 * j + which) * piece
                main = jnp.dot(act, pool[slot, pl.ds(base, depth)], preferred_element_type=f32)
                delta = jnp.dot(low[span], pool[slot, pl.ds(base + depth, 2 * width)], preferred_element_type=f32)
                parts.append(main + (lora_scale * delta).astype(bf16).astype(f32))
            gate, up = parts
            cols = pl.ds(pl.multiple_of(b * block + j * col, col), col)
            hid[span, cols] = (gate * jax.nn.sigmoid(gate) * up).astype(bf16)

    def x_wait(group, first):
        got = xs.at[pl.ds(first, (group + 1) * half - first)]
        pltpu.make_async_copy(got, got, x_recv.at[group]).wait()

    def wd_copy(j):
        slot = n_slots - 1 - j // per_slot
        start = (j % per_slot) * ff
        return pltpu.make_async_copy(wd_ref.at[:, pl.ds(pl.multiple_of(j * col, col), col)],
                                     pool.at[slot, pl.ds(start, ff)], wd_sem.at[j])

    near, far = pl.ds(0, half), pl.ds(half, half)
    small_wait(0, ag)
    small_wait(1, au)
    x_wait(0, same_rows)
    lowg[near] = low_rows(xs[near], ag, near)
    lowu[near] = low_rows(xs[near], au, near)

    @pl.loop(0, n_blocks)
    def _(b):
        load_wait(lax.rem(b, n_slots))
        gate_up(b, near)

        @pl.when(b < n_blocks - n_slots)
        def _():
            block_copies(b + n_slots, lax.rem(b, n_slots), 'all')

    x_wait(1, half)
    lowg[far] = low_rows(xs[far], ag, far)
    lowu[far] = low_rows(xs[far], au, far)

    @pl.loop(0, n_blocks)
    def _(i):
        b = n_blocks - 1 - i

        @pl.when(b < n_blocks - n_slots)
        def _():
            load_wait(lax.rem(b, n_slots))
        gate_up(b, far)

        @pl.when(i < n_blocks - n_slots)
        def _():
            block_copies(n_blocks - n_slots - 1 - i, lax.rem(b, n_slots), 'all')

        for k in range((n_cols + per_slot - 1) // per_slot):
            @pl.when(i == n_blocks - n_slots + k)
            def _():
                for j in range(k * per_slot, min((k + 1) * per_slot, n_cols)):
                    wd_copy(j).start()

    sent = send.at[pl.ds(same_rows, rows - same_rows)]
    pltpu.make_async_copy(sent, sent, x_send).wait()
    pltpu.make_async_copy(others, others, info_send).wait()
    small_wait(2, ad)
    small_wait(3, bd)
    every = pl.ds(0, rows)
    lowg[...] = low_rows(hid[...], ad, every)

    @pl.loop(0, n_cols)
    def _(j):
        slot = n_slots - 1 - j // per_slot
        start = pl.multiple_of(lax.rem(j, per_slot) * ff, 256)
        cols = pl.ds(pl.multiple_of(j * col, col), col)
        got = pool.at[slot, pl.ds(start, ff)]
        pltpu.make_async_copy(got, got, wd_sem.at[j]).wait()
        main = jnp.dot(hid[...], pool[slot, pl.ds(start, ff)], preferred_element_type=f32)
        delta = jnp.dot(lowg[...], bd[:, cols], preferred_element_type=f32)
        total = main + (lora_scale * delta).astype(bf16).astype(f32)
        send[:, cols] = (xs[:, cols].astype(f32) + total).astype(bf16)
        ret[pl.ds(0, same_rows), cols] = send[pl.ds(0, same_rows), cols]
        for seen in reversed(range(chips)):
            theirs = position[(chips - order[seen]) % chips]
            for kind in range(2):
                if seen == 0 and kind == 0:
                    continue
                count = cross_rows if kind else same_rows
                remote(send.at[pl.ds(seen * unit + kind * same_rows, count), cols],
                       ret.at[pl.ds(theirs * unit + kind * same_rows, count), cols],
                       out_send, out_recv, targets[seen][kind]).start()

    back = ret.at[pl.ds(same_rows, rows - same_rows)]
    pltpu.make_async_copy(back, back, out_recv).wait()
    o_ref[...] = lax.dot_general(perm, ret[...], (((0,), (0,)), ((), ())), preferred_element_type=f32).astype(bf16)
    pltpu.make_async_copy(sent, sent, out_send).wait()


def mlp_call(chips, rank, cross_rows, ident, x, ids, wg, wu, wd, ag, au, ad, bg, bu, bd):
    tok, depth = x.shape
    width = bg.shape[0]
    ff = wg.shape[1]
    rows = chips * (same_rows + cross_rows)
    n_sub = ff // n_blocks // col
    n_cols = depth // col
    slot_rows = max(2 * n_sub * (depth + 2 * width), ff)
    hbm, vmem = pl.BlockSpec(memory_space=pl.ANY), pl.BlockSpec(memory_space=pltpu.VMEM)
    bf16 = jnp.bfloat16
    dma = pltpu.SemaphoreType.DMA
    macs = rows * (3 * depth * ff + 2 * width * (2 * ff + depth) + 2 * width * (2 * depth + ff))
    return pl.pallas_call(
        functools.partial(mlp_kernel, chips, rank, cross_rows),
        out_shape=(jax.ShapeDtypeStruct((tok, depth), bf16), jax.ShapeDtypeStruct((1, tok), jnp.int32),
                   jax.ShapeDtypeStruct(bg.shape, bf16), jax.ShapeDtypeStruct(bu.shape, bf16), jax.ShapeDtypeStruct(bd.shape, bf16)),
        in_specs=[vmem, vmem] + [hbm] * 9,
        out_specs=(vmem, vmem, hbm, hbm, hbm),
        scratch_shapes=[
            pltpu.VMEM((n_slots, slot_rows, col), bf16),
            pltpu.VMEM((rows, depth), bf16), pltpu.VMEM((rows, depth), bf16), pltpu.VMEM((rows, depth), bf16),
            pltpu.VMEM((rows, ff), bf16),
            pltpu.VMEM((rows, 2 * width), bf16), pltpu.VMEM((rows, 2 * width), bf16), pltpu.VMEM((rows, 2 * width), bf16),
            pltpu.VMEM((2 * width, depth), bf16), pltpu.VMEM((2 * width, depth), bf16), pltpu.VMEM((2 * width, ff), bf16),
            pltpu.VMEM((2 * width, depth), bf16),
            pltpu.VMEM((2 * chips, 1, tok), jnp.int32),
            dma((n_slots,)), dma((n_cols,)), dma((4,)), dma((6,)), dma, dma((2,)), dma, dma, dma, dma,
        ],
        compiler_params=pltpu.CompilerParams(collective_id=ident, has_side_effects=True, vmem_limit_bytes=66_900_000),
        cost_estimate=pl.CostEstimate(flops=2 * macs, bytes_accessed=6 * depth * ff, transcendentals=rows * ff),
        name='mlp_%d' % cross_rows,
    )(x, ids, wg, wu, wd, ag, au, ad, bg, bu, bd)


base_rows = 16
extra_rows = 32


def lane_kernel(chips, rank, x_ref, id_ref, wg_ref, wu_ref, wd_ref, ag_ref, au_ref, ad_ref, bg_ref, bu_ref, bd_ref,
                o_ref, flag_ref, pg_ref, pu_ref, pd_ref,
                pool, xs, send, stage, ret, hid, lowg, lowu, mask, valid, ag, au, ad, bd, info, merge,
                load_sem, wd_sem, small_sem, pair_send, pair_recv, base_send, base_recv, extra_send, extra_recv,
                info_send, info_recv, out_send, out_recv, merge_send, merge_recv):
    order = ring_order(chips)
    position = {step: place for place, step in enumerate(order)}
    tok, depth = x_ref.shape
    width = bg_ref.shape[0]
    ff = wg_ref.shape[1]
    block = ff // n_blocks
    n_sub = block // col
    piece = depth + 2 * width
    used = 2 * n_sub * piece
    per_chip = 2 * (width // rank)
    n_cols = depth // col
    per_slot = pool.shape[1] // ff
    last = chips // 2
    near_base, near_extra = last + 1, 3
    first_extra = near_base * base_rows
    end_extra = first_extra + chips * extra_rows
    rows = end_extra + (chips - near_base) * base_rows
    split = first_extra + near_extra * extra_rows
    slots_base = chips * base_rows
    slots = slots_base + extra_rows
    part = extra_rows // 2
    f32, bf16 = jnp.float32, jnp.bfloat16

    def base_at(seen):
        return seen * base_rows if seen < near_base else end_extra + (seen - near_base) * base_rows

    def extra_at(seen):
        return first_extra + seen * extra_rows

    me = lax.axis_index('data')
    core = lax.rem(me, 2)
    chip = me // 2
    partner = me + 1 - 2 * core
    lane = [2 * lax.rem(chip + step, chips) + core for step in order]
    cross = [2 * lax.rem(chip + step, chips) + 1 - core for step in order]
    up, down = lane[1], lane[2]
    peers = lane[1:] + cross

    barrier = pltpu.get_barrier_semaphore()
    for peer in peers:
        pl.semaphore_signal(barrier, inc=1, device_id={'data': peer}, device_id_type=pl.DeviceIdType.MESH)

    def block_copies(b, slot, which_part):
        for j in range(n_sub):
            cols = pl.ds(pl.multiple_of(b * block + j * col, col), col)
            for which, (w, own, far) in enumerate(((wg_ref, bg_ref, pg_ref), (wu_ref, bu_ref, pu_ref))):
                base = (2 * j + which) * piece
                todo = []
                if which_part != 'pair':
                    todo += [(w, base, depth), (own, base + depth, width)]
                if which_part != 'own':
                    todo += [(far, base + depth + width, width)]
                for src, start, count in todo:
                    pltpu.make_async_copy(src.at[:, cols], pool.at[slot, pl.ds(start, count)], load_sem.at[slot]).start()

    def load_wait(slot):
        whole = pool.at[slot, pl.ds(0, used)]
        pltpu.make_async_copy(whole, whole, load_sem.at[slot]).wait()

    def remote(src, dst, s_sem, r_sem, dev):
        return pltpu.make_async_remote_copy(src_ref=src, dst_ref=dst, send_sem=s_sem, recv_sem=r_sem,
                                            device_id={'data': dev}, device_id_type=pl.DeviceIdType.MESH)

    def await_bytes(ref, sem):
        pltpu.make_async_copy(ref, ref, sem).wait()

    for b in range(n_slots):
        block_copies(b, b, 'own')
    own_a = pl.ds(pl.multiple_of(me * width, width), width)
    far_a = pl.ds(pl.multiple_of(partner * width, width), width)
    for k, (src, dst) in enumerate(((ag_ref, ag), (au_ref, au), (ad_ref, ad))):
        pltpu.make_async_copy(src.at[own_a], dst.at[pl.ds(0, width)], small_sem.at[k]).start()
        pltpu.make_async_copy(src.at[far_a], dst.at[pl.ds(width, width)], small_sem.at[k]).start()
    pltpu.make_async_copy(bd_ref, bd.at[pl.ds(0, width)], small_sem.at[3]).start()

    ids = id_ref[...]
    step = lax.rem(ids // per_chip - chip + chips, chips)
    place = jnp.where(step < last, jnp.maximum(2 * step - 1, 0), jnp.where(step == last, chips - 1, 2 * (chips - step)))
    hot = (lax.broadcasted_iota(jnp.int32, (2 * chips, tok), 0) == place).astype(f32)
    before = (lax.broadcasted_iota(jnp.int32, (tok, tok), 0) < lax.broadcasted_iota(jnp.int32, (tok, tok), 1)).astype(f32).astype(bf16)
    counts = jnp.dot(hot.astype(bf16), before, preferred_element_type=f32)
    order_in = jnp.sum(hot * counts, axis=0, keepdims=True)
    spill = jnp.broadcast_to((order_in >= base_rows).astype(f32), (2 * chips, tok))
    spilled = jnp.dot(spill.astype(bf16), before, preferred_element_type=f32)[:1].astype(jnp.int32)
    order_in = order_in.astype(jnp.int32)
    slot_of = jnp.where(order_in < base_rows, place * base_rows + order_in, slots_base + spilled)
    info[0] = slot_of * (per_chip * chips) + ids
    perm = (lax.broadcasted_iota(jnp.int32, (slots, tok), 0) == slot_of).astype(f32).astype(bf16)
    send[...] = jnp.dot(perm, x_ref[...], preferred_element_type=f32).astype(bf16)
    xs[pl.ds(0, base_rows)] = send[pl.ds(0, base_rows)]
    xs[pl.ds(extra_at(0), extra_rows)] = send[pl.ds(slots_base, extra_rows)]

    pl.semaphore_wait(barrier, len(peers))

    for to, step_to in enumerate(order):
        seen = position[(chips - step_to) % chips]
        if to:
            remote(info.at[0], info.at[2 * seen], info_send, info_recv, lane[to]).start()
        remote(info.at[0], info.at[2 * seen + 1], info_send, info_recv, cross[to]).start()

    def pass_on(hop, start):
        for way, dev in ((0, up), (1, down)):
            src_seen = 0 if hop == 0 else position[(chips - hop) % chips if way == 0 else hop]
            dst_seen = position[(chips - hop - 1) % chips if way == 0 else hop + 1]
            first, count = (way * part, part) if hop == last - 1 else (0, extra_rows)
            src = send.at[pl.ds(slots_base, extra_rows)] if hop == 0 else xs.at[pl.ds(extra_at(src_seen) + first, count)]
            if hop and start:
                whole = xs.at[pl.ds(extra_at(src_seen), extra_rows)]
                await_bytes(whole, extra_recv.at[way, hop - 1])
            remote(src, xs.at[pl.ds(extra_at(dst_seen) + first, count)], extra_send, extra_recv.at[way, hop], dev).start()

    pass_on(0, True)
    pair_copies = []
    for b in range(n_blocks):
        cols = pl.ds(b * block, block)
        pair_copies.append(remote(bg_ref.at[:, cols], pg_ref.at[:, cols], pair_send.at[2 * b], pair_recv.at[2 * b], partner))
        pair_copies.append(remote(bu_ref.at[:, cols], pu_ref.at[:, cols], pair_send.at[2 * b + 1], pair_recv.at[2 * b + 1], partner))
    pair_copies.append(remote(bd_ref, pd_ref, pair_send.at[2 * n_blocks], pair_recv.at[2 * n_blocks], partner))
    for c in pair_copies:
        c.start()
    for to, step_to in enumerate(order):
        seen = position[(chips - step_to) % chips]
        if to:
            remote(send.at[pl.ds(to * base_rows, base_rows)], xs.at[pl.ds(base_at(seen), base_rows)],
                   base_send, base_recv.at[int(seen >= near_base)], lane[to]).start()

    def pair_wait(b):
        cols = pl.ds(pl.multiple_of(b * block, col), block)
        await_bytes(pg_ref.at[:, cols], pair_recv.at[2 * b])
        await_bytes(pu_ref.at[:, cols], pair_recv.at[2 * b + 1])

    await_bytes(info.at[pl.ds(1, 2 * chips - 1)], info_recv)
    flag = jnp.zeros((1, tok), jnp.int32)
    for other in range(2 * chips):
        flag = jnp.maximum(flag, (info[other] // (per_chip * chips) >= slots).astype(jnp.int32))
    flag_ref[...] = flag
    for seen, step_from in enumerate(order):
        theirs = position[(chips - step_from) % chips]
        code = info[2 * seen]
        theirs_slot = code // (per_chip * chips)
        adapter = lax.rem(code, per_chip * chips)
        pick_id = jnp.where(adapter // per_chip == chip, lax.rem(lax.rem(adapter, per_chip) + core * (width // rank), per_chip) + 1, 0)
        for at, start, count in ((base_at(seen), theirs * base_rows, base_rows), (extra_at(seen), slots_base, extra_rows)):
            hit = lax.broadcasted_iota(jnp.int32, (count, tok), 0) + start == theirs_slot
            pick = jnp.sum(jnp.where(hit, pick_id, 0), axis=1, keepdims=True)
            lane_id = lax.broadcasted_iota(jnp.int32, (count, 2 * width), 1) // rank + 1
            mask[pl.ds(at, count)] = (lane_id == pick).astype(f32).astype(bf16)
            if count == extra_rows:
                valid[pl.ds(at - first_extra, count)] = jnp.broadcast_to((pick > 0).astype(f32), (count, col))

    pair_wait(0)
    block_copies(0, 0, 'pair')
    pass_on(1, True)

    def low_rows(act, a, span):
        low = lax.dot_general(act, a[...], (((1,), (1,)), ((), ())), preferred_element_type=f32)
        return low.astype(bf16) * mask[span]

    def gate_up(b, span):
        slot = lax.rem(b, n_slots)
        act = xs[span]
        for j in range(n_sub):
            parts = []
            for which, low in enumerate((lowg, lowu)):
                base = (2 * j + which) * piece
                main = jnp.dot(act, pool[slot, pl.ds(base, depth)], preferred_element_type=f32)
                delta = jnp.dot(low[span], pool[slot, pl.ds(base + depth, 2 * width)], preferred_element_type=f32)
                parts.append(main + (lora_scale * delta).astype(bf16).astype(f32))
            gate, up_act = parts
            cols = pl.ds(pl.multiple_of(b * block + j * col, col), col)
            hid[span, cols] = (gate * jax.nn.sigmoid(gate) * up_act).astype(bf16)

    def wd_copy(j):
        slot = n_slots - 1 - j // per_slot
        start = (j % per_slot) * ff
        return pltpu.make_async_copy(wd_ref.at[:, pl.ds(pl.multiple_of(j * col, col), col)],
                                     pool.at[slot, pl.ds(start, ff)], wd_sem.at[j])

    near, far = pl.ds(0, split), pl.ds(split, rows - split)
    await_bytes(ag, small_sem.at[0])
    await_bytes(au, small_sem.at[1])
    await_bytes(xs.at[pl.ds(base_rows, first_extra - base_rows)], base_recv.at[0])
    for b in range(1, n_slots):
        pair_wait(b)
        block_copies(b, b, 'pair')
    lowg[near] = low_rows(xs[near], ag, near)
    lowu[near] = low_rows(xs[near], au, near)

    @pl.loop(0, n_blocks)
    def _(b):
        load_wait(lax.rem(b, n_slots))
        gate_up(b, near)
        for hop in range(2, last):
            @pl.when(b == 2 * hop - 3)
            def _():
                pass_on(hop, True)

        @pl.when(b < n_blocks - n_slots)
        def _():
            pair_wait(b + n_slots)
            block_copies(b + n_slots, lax.rem(b, n_slots), 'all')

    final = position[last]
    for way in range(2):
        await_bytes(xs.at[pl.ds(extra_at(final) + way * part, part)], extra_recv.at[way, last - 1])
    await_bytes(xs.at[pl.ds(end_extra, rows - end_extra)], base_recv.at[1])
    lowg[far] = low_rows(xs[far], ag, far)
    lowu[far] = low_rows(xs[far], au, far)

    @pl.loop(0, n_blocks)
    def _(i):
        b = n_blocks - 1 - i

        @pl.when(b < n_blocks - n_slots)
        def _():
            load_wait(lax.rem(b, n_slots))
        gate_up(b, far)

        @pl.when(i < n_blocks - n_slots)
        def _():
            block_copies(n_blocks - n_slots - 1 - i, lax.rem(b, n_slots), 'all')

        for k in range((n_cols + per_slot - 1) // per_slot):
            @pl.when(i == n_blocks - n_slots + k)
            def _():
                for j in range(k * per_slot, min((k + 1) * per_slot, n_cols)):
                    wd_copy(j).start()

    await_bytes(pd_ref, pair_recv.at[2 * n_blocks])
    pd_load = pltpu.make_async_copy(pd_ref, bd.at[pl.ds(width, width)], small_sem.at[3])
    pd_load.start()
    await_bytes(ad, small_sem.at[2])
    lowg[...] = low_rows(hid[...], ad, pl.ds(0, rows))
    await_bytes(bd, small_sem.at[3])

    def down_cols(j, pieces):
        slot = n_slots - 1 - j // per_slot
        start = pl.multiple_of(lax.rem(j, per_slot) * ff, col)
        cols = pl.ds(pl.multiple_of(j * col, col), col)

        def take(ref, c):
            got = [ref[p, c] for p in pieces]
            return got[0] if len(got) == 1 else jnp.concatenate(got, axis=0)
        every = slice(None)
        main = jnp.dot(take(hid, every), pool[slot, pl.ds(start, ff)], preferred_element_type=f32)
        delta = jnp.dot(take(lowg, every), bd[:, cols], preferred_element_type=f32)
        return take(xs, cols).astype(f32) + (main + (lora_scale * delta).astype(bf16).astype(f32)), cols

    def merge_step(hop, j):
        cols = pl.ds(pl.multiple_of(j * col, col), col)
        for way, dev in ((0, up), (1, down)):
            home = position[last - hop if way == 0 else (chips - last + hop) % chips]
            at = extra_at(home)
            first, count = (way * part, part) if hop == 0 else (0, extra_rows)
            if hop:
                f, c = (way * part, part) if hop == 1 else (0, extra_rows)
                got = merge.at[way, hop - 1, pl.ds(f, c), cols]
                await_bytes(got, merge_recv.at[way, hop - 1, j])
                mine = pl.ds(at + f, c)
                stage[mine, cols] = stage[mine, cols] + merge[way, hop - 1, pl.ds(f, c), cols]
            remote(stage.at[pl.ds(at + first, count), cols], merge.at[way, hop, pl.ds(first, count), cols],
                   merge_send, merge_recv.at[way, hop, j], dev).start()

    def merge_steps(turn):
        for hop in range(1, last):
            t = turn - 2 * hop

            @pl.when((t >= 0) & (t < n_cols))
            def _():
                merge_step(hop, t)

    @pl.loop(0, n_cols)
    def _(j):
        cols = pl.ds(pl.multiple_of(j * col, col), col)
        got = pool.at[n_slots - 1 - j // per_slot, pl.ds(pl.multiple_of(lax.rem(j, per_slot) * ff, col), ff)]
        await_bytes(got, wd_sem.at[j])
        total, _ = down_cols(j, [pl.ds(first_extra, chips * extra_rows)])
        stage[pl.ds(first_extra, chips * extra_rows), cols] = jnp.where(valid[...] > 0, total, 0.0).astype(bf16)
        merge_step(0, j)
        merge_steps(j)

    @pl.loop(0, n_cols)
    def _(j):
        total, cols = down_cols(j, [pl.ds(0, first_extra), pl.ds(end_extra, rows - end_extra)])
        total = total.astype(bf16)
        stage[pl.ds(0, first_extra), cols] = total[:first_extra]
        stage[pl.ds(end_extra, rows - end_extra), cols] = total[first_extra:]
        ret[pl.ds(0, base_rows), cols] = total[:base_rows]
        for seen in reversed(range(1, chips)):
            theirs = position[(chips - order[seen]) % chips]
            remote(stage.at[pl.ds(base_at(seen), base_rows), cols], ret.at[pl.ds(theirs * base_rows, base_rows), cols],
                   out_send, out_recv, lane[seen]).start()
        merge_steps(j + n_cols)

    for turn in range(2 * n_cols, n_cols + 2 * (last - 1)):
        for hop in range(1, last):
            if 0 <= turn - 2 * hop < n_cols:
                merge_step(hop, turn - 2 * hop)
    for j in range(n_cols):
        cols = pl.ds(j * col, col)
        for way in range(2):
            await_bytes(merge.at[way, last - 1, pl.ds(0, extra_rows), cols], merge_recv.at[way, last - 1, j])
    ret[pl.ds(slots_base, extra_rows)] = stage[pl.ds(extra_at(0), extra_rows)] + (merge[0, last - 1] + merge[1, last - 1])
    await_bytes(ret.at[pl.ds(base_rows, slots_base - base_rows)], out_recv)
    o_ref[...] = lax.dot_general(perm, ret[...], (((0,), (0,)), ((), ())), preferred_element_type=f32).astype(bf16)

    for c in pair_copies:
        c.wait_send()
    await_bytes(info.at[pl.ds(1, 2 * chips - 1)], info_send)
    await_bytes(send.at[pl.ds(base_rows, slots_base - base_rows)], base_send)
    await_bytes(xs.at[pl.ds(0, (2 * last - 1) * extra_rows)], extra_send)
    await_bytes(ret.at[pl.ds(base_rows, slots_base - base_rows)], out_send)
    await_bytes(stage.at[pl.ds(0, (2 * last - 1) * extra_rows)], merge_send)


def lane_call(chips, rank, ident, x, ids, wg, wu, wd, ag, au, ad, bg, bu, bd):
    tok, depth = x.shape
    width = bg.shape[0]
    ff = wg.shape[1]
    rows = chips * (base_rows + extra_rows)
    slots = chips * base_rows + extra_rows
    n_sub = ff // n_blocks // col
    n_cols = depth // col
    slot_rows = max(2 * n_sub * (depth + 2 * width), ff)
    hbm, vmem = pl.BlockSpec(memory_space=pl.ANY), pl.BlockSpec(memory_space=pltpu.VMEM)
    bf16 = jnp.bfloat16
    dma = pltpu.SemaphoreType.DMA
    macs = rows * (3 * depth * ff + 2 * width * (2 * ff + depth) + 2 * width * (2 * depth + ff))
    low = pltpu.VMEM((rows, 2 * width), bf16)
    a_buf = pltpu.VMEM((2 * width, depth), bf16)
    return pl.pallas_call(
        functools.partial(lane_kernel, chips, rank),
        out_shape=(jax.ShapeDtypeStruct((tok, depth), bf16), jax.ShapeDtypeStruct((1, tok), jnp.int32),
                   jax.ShapeDtypeStruct(bg.shape, bf16), jax.ShapeDtypeStruct(bu.shape, bf16), jax.ShapeDtypeStruct(bd.shape, bf16)),
        in_specs=[vmem, vmem] + [hbm] * 9,
        out_specs=(vmem, vmem, hbm, hbm, hbm),
        scratch_shapes=[
            pltpu.VMEM((n_slots, slot_rows, col), bf16),
            pltpu.VMEM((rows, depth), bf16), pltpu.VMEM((slots, depth), bf16), pltpu.VMEM((rows, depth), bf16), pltpu.VMEM((slots, depth), bf16),
            pltpu.VMEM((rows, ff), bf16),
            low, low, low, pltpu.VMEM((chips * extra_rows, col), jnp.float32),
            a_buf, a_buf, pltpu.VMEM((2 * width, ff), bf16), a_buf,
            pltpu.VMEM((2 * chips, 1, tok), jnp.int32),
            pltpu.VMEM((2, chips // 2, extra_rows, depth), bf16),
            dma((n_slots,)), dma((n_cols,)), dma((4,)), dma((2 * n_blocks + 1,)), dma((2 * n_blocks + 1,)), dma, dma((2,)), dma, dma((2, chips // 2)),
            dma, dma, dma, dma, dma, dma((2, chips // 2, n_cols)),
        ],
        compiler_params=pltpu.CompilerParams(collective_id=ident, has_side_effects=True, vmem_limit_bytes=66_900_000),
        cost_estimate=pl.CostEstimate(flops=2 * macs, bytes_accessed=6 * depth * ff, transcendentals=rows * ff),
        name='mlp_lane',
    )(x, ids, wg, wu, wd, ag, au, ad, bg, bu, bd)


def solution(mesh):
    groups = mesh.shape['data']
    row_spec = P(('rep', 'data'), None)
    tok_spec = P(('rep', 'data'))
    full_two = P(None, None)
    full_three = P(None, None, None)
    owned = P('data', None, None)

    def device_fn(hidden, adapter_id, w_gate, w_up, w_down, a_gate, b_gate, a_up, b_up, a_down, b_down):
        rank = b_gate.shape[1]

        def rank_rows(a):
            return jnp.swapaxes(a, 1, 2).reshape(-1, a.shape[1])

        def flat(b):
            return b.reshape(-1, b.shape[2])

        args = (hidden, adapter_id.reshape(1, -1), w_gate, w_up, w_down, rank_rows(a_gate), rank_rows(a_up), rank_rows(a_down),
                flat(b_gate), flat(b_up), flat(b_down))
        fast, flag = lane_call(groups // 2, rank, 0, *args)[:2]
        return lax.cond(jnp.max(flag) > 0, lambda *a: mlp_call(groups // 2, rank, same_rows, 1, *a)[0], lambda *a: fast, *args)

    return jax.shard_map(device_fn, mesh=mesh, in_specs=(row_spec, tok_spec, full_two, full_two, full_two, full_three, owned, full_three, owned, full_three, owned), out_specs=row_spec, check_vma=False)
```
